8 devices in a mesh: exam: 2 (over z, y), rows: 4 (over x, core).
Axes of the slice: x: 2, y: 2, z: 1, core: 2. Of those that a mesh axis runs over, the one named last changes fastest.
Arguments:
- kspace: float32 [2, 8, 8192], P(None, None, ('exam', 'rows')), parts along dimension 2
- weight_row: float32 [6, 8192], P(None, ('exam', 'rows')), parts along dimension 1
- weight_col: float32 [6, 8192], P(None, ('exam', 'rows')), parts along dimension 1
- row_idx: int32 [8192], P(('exam', 'rows')), parts along dimension 0
- col_idx: int32 [8192], P(('exam', 'rows')), parts along dimension 0
- counts: int32 [8], P(('exam', 'rows')), parts along dimension 0
- coil_maps: float32 [2, 8, 384, 768], P(None, None, None, ('exam', 'rows')), parts along dimension 3
- deapod: float32 [384], replicated
Outputs:
- output: float32 [2, 768, 384], P(None, ('exam', 'rows')), parts along dimension 1
There are 2 independent parts. The reference program is written for one: setup_inputs(seed, part) draws one part's arguments, and reference() takes and returns one part's arrays. A program takes and returns all parts, laid end to end along the dimension named above; an argument that names none is the same for every part.
All inputs are finite; a program needn't handle non-finite values.
Results may differ from the reference program's by a relative error of at most 0.001.
Values are sent between devices in bfloat16 or wider.
A program may use at most 1 GiB of HBM per device.

```python
import math
import jax
import jax.numpy as jnp
from jax import lax

IMG_SIZE = 384
NUM_COILS = 8
KERNEL_WIDTH = 6
ROW_BLOCKS = 4
SAMPLES_DEV = 1024

GRID_SIZE = 2 * IMG_SIZE
BLOCK_ROWS = GRID_SIZE // ROW_BLOCKS
HALF_WIDTH = KERNEL_WIDTH // 2
SAMPLES_ALL = ROW_BLOCKS * SAMPLES_DEV


def draw_layout(key):
    key_count, key_one, key_two, key_three, key_left, key_right = jax.random.split(key, 6)
    block_ids = jnp.arange(ROW_BLOCKS, dtype=jnp.int32)
    distance = jnp.abs(2 * block_ids + 1 - ROW_BLOCKS) // 2
    base_count = jnp.maximum(SAMPLES_DEV // (1 + distance), SAMPLES_DEV // 8)
    jitter = jax.random.randint(key_count, (ROW_BLOCKS,), 0, base_count // 2 + 1)
    jitter = jnp.where(block_ids == ROW_BLOCKS // 2, 0, jitter)
    counts = (base_count - jitter).astype(jnp.int32)
    slot_shape = (ROW_BLOCKS, SAMPLES_DEV)
    draw_one = jax.random.randint(key_one, slot_shape, 0, BLOCK_ROWS)
    draw_two = jax.random.randint(key_two, slot_shape, 0, BLOCK_ROWS)
    draw_three = jax.random.randint(key_three, slot_shape, 0, BLOCK_ROWS)
    offset = ((draw_one * draw_two) // BLOCK_ROWS * draw_three) // BLOCK_ROWS
    local_row = jnp.where(block_ids[:, None] < ROW_BLOCKS // 2, BLOCK_ROWS - 1 - offset, offset)
    row_idx = (block_ids[:, None] * BLOCK_ROWS + local_row).reshape(SAMPLES_ALL).astype(jnp.int32)
    col_left = jax.random.randint(key_left, (SAMPLES_ALL,), 0, IMG_SIZE + 1)
    col_right = jax.random.randint(key_right, (SAMPLES_ALL,), 0, IMG_SIZE)
    col_idx = ((IMG_SIZE + col_left - col_right) % GRID_SIZE).astype(jnp.int32)
    return counts, row_idx, col_idx


def setup_inputs(seed: int = 0, part: int = 0) -> dict:
    base_key = jax.random.key(seed)
    part_key = jax.random.fold_in(base_key, part)
    key_layout, key_kspace, key_wrow, key_wcol, key_maps = jax.random.split(part_key, 5)
    key_deapod = jax.random.fold_in(base_key, 1000003)
    counts, row_idx, col_idx = draw_layout(key_layout)
    radius = (jnp.abs(row_idx - IMG_SIZE) + jnp.abs(col_idx - IMG_SIZE)).astype(jnp.float32) / GRID_SIZE
    amplitude = 1.0 / (1.0 + 16.0 * radius)
    raw_kspace = jax.random.normal(key_kspace, (2, NUM_COILS, SAMPLES_ALL), jnp.float32) * amplitude[None, None, :]
    energy = jnp.sum(raw_kspace * raw_kspace, axis=(0, 2), keepdims=True)
    kspace = raw_kspace / jnp.sqrt(energy)
    tap_pos = jnp.arange(KERNEL_WIDTH, dtype=jnp.float32) - (KERNEL_WIDTH - 1) / 2.0
    bell_shape = jnp.exp(-(tap_pos / (0.5 * KERNEL_WIDTH)) ** 2)[:, None] / math.sqrt(KERNEL_WIDTH)
    weight_row = bell_shape * (0.6 + 0.8 * jax.random.uniform(key_wrow, (KERNEL_WIDTH, SAMPLES_ALL), jnp.float32))
    weight_col = bell_shape * (0.6 + 0.8 * jax.random.uniform(key_wcol, (KERNEL_WIDTH, SAMPLES_ALL), jnp.float32))
    coil_maps = jax.random.normal(key_maps, (2, NUM_COILS, IMG_SIZE, IMG_SIZE), jnp.float32) / math.sqrt(2.0 * NUM_COILS)
    pixel_pos = (jnp.arange(IMG_SIZE, dtype=jnp.float32) - IMG_SIZE / 2.0) / IMG_SIZE
    deapod = (1.0 + 2.0 * pixel_pos * pixel_pos) * (0.8 + 0.4 * jax.random.uniform(key_deapod, (IMG_SIZE,), jnp.float32))
    return {'kspace': kspace, 'weight_row': weight_row, 'weight_col': weight_col, 'row_idx': row_idx, 'col_idx': col_idx, 'counts': counts, 'coil_maps': coil_maps, 'deapod': deapod}


def dft_table():
    frequency = jnp.arange(GRID_SIZE, dtype=jnp.int32)[:, None] - IMG_SIZE
    pixel_pos = jnp.arange(IMG_SIZE, dtype=jnp.int32)[None, :] - IMG_SIZE // 2
    angle_rad = ((frequency * pixel_pos) % GRID_SIZE).astype(jnp.float32) * (2.0 * math.pi / GRID_SIZE)
    cos_tab = jnp.cos(angle_rad).astype(jnp.bfloat16).astype(jnp.float32)
    sin_tab = jnp.sin(angle_rad).astype(jnp.bfloat16).astype(jnp.float32)
    return cos_tab, sin_tab


def spread_grid(kspace, weight_row, weight_col, row_idx, col_idx, counts):
    tap_offsets = jnp.arange(KERNEL_WIDTH, dtype=jnp.int32) - HALF_WIDTH
    slot_ids = jnp.arange(SAMPLES_DEV, dtype=jnp.int32)
    keep_all = (slot_ids[None, :] < counts[:, None]).astype(jnp.float32)
    blk_kspace = jnp.moveaxis(kspace.reshape(2, NUM_COILS, ROW_BLOCKS, SAMPLES_DEV), 2, 0)
    blk_wrow = jnp.moveaxis(weight_row.reshape(KERNEL_WIDTH, ROW_BLOCKS, SAMPLES_DEV), 1, 0)
    blk_wcol = jnp.moveaxis(weight_col.reshape(KERNEL_WIDTH, ROW_BLOCKS, SAMPLES_DEV), 1, 0)
    blk_rows = row_idx.reshape(ROW_BLOCKS, SAMPLES_DEV)
    blk_cols = col_idx.reshape(ROW_BLOCKS, SAMPLES_DEV)

    def add_block(grid_acc, blk_data):
        ks_vals, wrow_vals, wcol_vals, rows_vals, cols_vals, keep_vals = blk_data
        grid_rows = (rows_vals[:, None] + tap_offsets[None, :]) % GRID_SIZE
        grid_cols = (cols_vals[:, None] + tap_offsets[None, :]) % GRID_SIZE
        flat_pos = (grid_rows[:, :, None] * GRID_SIZE + grid_cols[:, None, :]).reshape(-1)
        weight = (wrow_vals.T * keep_vals[:, None])[:, :, None] * wcol_vals.T[:, None, :]
        contrib = ks_vals[:, :, :, None, None] * weight[None, None]
        grid_acc = grid_acc.at[:, :, flat_pos].add(contrib.reshape(2, NUM_COILS, -1))
        return grid_acc, None

    grid_init = jnp.zeros((2, NUM_COILS, GRID_SIZE * GRID_SIZE), jnp.float32)
    grid_flat = lax.scan(add_block, grid_init, (blk_kspace, blk_wrow, blk_wcol, blk_rows, blk_cols, keep_all))[0]
    return grid_flat.reshape(2, NUM_COILS, GRID_SIZE, GRID_SIZE)


def reference(kspace, weight_row, weight_col, row_idx, col_idx, counts, coil_maps, deapod):
    grid_bf = spread_grid(kspace, weight_row, weight_col, row_idx, col_idx, counts).astype(jnp.bfloat16).astype(jnp.float32)
    cos_tab, sin_tab = dft_table()
    grid_re = grid_bf[0]
    grid_im = grid_bf[1]
    half_re = jnp.einsum('cuv,vj->cuj', grid_re, cos_tab) - jnp.einsum('cuv,vj->cuj', grid_im, sin_tab)
    half_im = jnp.einsum('cuv,vj->cuj', grid_re, sin_tab) + jnp.einsum('cuv,vj->cuj', grid_im, cos_tab)
    half_re = half_re.astype(jnp.bfloat16).astype(jnp.float32)
    half_im = half_im.astype(jnp.bfloat16).astype(jnp.float32)
    img_re = jnp.einsum('ui,cuj->cij', cos_tab, half_re) - jnp.einsum('ui,cuj->cij', sin_tab, half_im)
    img_im = jnp.einsum('ui,cuj->cij', sin_tab, half_re) + jnp.einsum('ui,cuj->cij', cos_tab, half_im)
    out_re = jnp.sum(coil_maps[0] * img_re + coil_maps[1] * img_im, axis=0)
    out_im = jnp.sum(coil_maps[0] * img_im - coil_maps[1] * img_re, axis=0)
    pix_scale = deapod[:, None] * deapod[None, :]
    return jnp.stack([out_re * pix_scale, out_im * pix_scale])
```

```python
import functools
import math

import jax
import jax.numpy as jnp
import numpy as np
from jax import lax
from jax.experimental import pallas as pl
from jax.experimental.pallas import tpu as pltpu
from jax.sharding import PartitionSpec as P

MESH = pl.DeviceIdType.MESH
F32 = jnp.float32
BF16 = jnp.bfloat16
LANES = 128
SUB = 8


def dft_tables(img_size, row_devs):
    grid_size = 2 * img_size
    frequency = np.arange(grid_size)[None, :] - img_size
    pixel_pos = np.arange(img_size)[:, None] - img_size // 2
    angle = ((frequency * pixel_pos) % grid_size).astype(np.float64) * (2.0 * math.pi / grid_size)
    table = np.stack([np.cos(angle), np.sin(angle)]).astype(np.float32).astype(jnp.bfloat16)
    block = grid_size // row_devs
    order = np.concatenate([np.arange(SUB, block - SUB), np.arange(SUB), np.arange(block - SUB, block)])
    by_core = []
    for core in range(2):
        rows = np.concatenate([(2 * chip + core) * block + order for chip in range(row_devs // 2)])
        by_core.append(table[:, :, rows])
    return table, np.stack(by_core)


def grid_kernel(data_ref, tab_hbm, h_ref, edge_ref, acc_a, acc_b, lvec, addr_v, gbuf, tab_v, addr_s, tab_sem, addr_sem, *, pitch, cols):
    chip = lax.axis_index('rows') // 2
    groups = acc_a.shape[0] // pitch
    half = tab_v.shape[1] // 2
    tab_copy = pltpu.make_async_copy(tab_hbm.at[:, pl.ds(pl.multiple_of(chip * 2 * half, 2 * half), 2 * half), :], tab_v, tab_sem)
    tab_copy.start()
    addr_v[...] = data_ref[24:32, :].astype(jnp.int32)
    addr_copy = pltpu.make_async_copy(addr_v, addr_s, addr_sem)
    addr_copy.start()

    @pl.loop(0, groups)
    def _(g):
        base = pl.multiple_of(g * pitch, SUB)
        acc_a[pl.ds(base, pitch), :] = jnp.zeros((pitch, LANES), F32)
        acc_b[pl.ds(base, pitch), :] = jnp.zeros((pitch, LANES), F32)

    addr_copy.wait()
    count = addr_s[7, 0]
    slot = lax.broadcasted_iota(jnp.int32, (2 * SUB, LANES), 0).astype(F32)
    tap_row = lax.broadcasted_iota(jnp.int32, (SUB, LANES), 0)

    @pl.loop(0, (count + LANES - 1) // LANES)
    def _(blk):
        first = pl.multiple_of(blk * LANES, LANES)
        wr8 = data_ref[16:24, pl.ds(first, LANES)]
        tap = slot - wr8[6:7, :]
        wrs = jnp.where(tap == 0.0, wr8[0:1, :], 0.0)
        for a in range(1, 6):
            wrs = wrs + jnp.where(tap == float(a), wr8[a:a + 1, :], 0.0)
        y16 = data_ref[0:16, pl.ds(first, LANES)]
        for part in range(2):
            w_part = wrs[part * SUB:(part + 1) * SUB, :]
            full = jnp.concatenate([y16[ch:ch + 1, :] * w_part for ch in range(16)], axis=0)
            lvec[:, part * LANES:(part + 1) * LANES] = full.T
        wc8 = jnp.where(tap_row < 6, data_ref[24:32, pl.ds(first, LANES)], 0.0)

        def contribution(k):
            wide = jnp.broadcast_to(wc8[:, k:k + 1], (SUB, LANES))
            lo = jnp.broadcast_to(lvec[k:k + 1, 0:LANES], (SUB, LANES))
            hi = jnp.broadcast_to(lvec[k:k + 1, LANES:2 * LANES], (SUB, LANES))
            return wide * lo, wide * hi

        for k in range(0, LANES, 2):
            at_a = addr_s[6, first + k]
            at_b = addr_s[6, first + k + 1]
            a_lo, a_hi = contribution(k)
            b_lo, b_hi = contribution(k + 1)
            old_a_lo = acc_a[pl.ds(at_a, SUB), :]
            old_a_hi = acc_a[pl.ds(at_a + pitch, SUB), :]
            old_b_lo = acc_b[pl.ds(at_b, SUB), :]
            old_b_hi = acc_b[pl.ds(at_b + pitch, SUB), :]
            acc_a[pl.ds(at_a, SUB), :] = old_a_lo + a_lo
            acc_a[pl.ds(at_a + pitch, SUB), :] = old_a_hi + a_hi
            acc_b[pl.ds(at_b, SUB), :] = old_b_lo + b_lo
            acc_b[pl.ds(at_b + pitch, SUB), :] = old_b_hi + b_hi

    def rows_sum(g, start, size):
        at = pl.multiple_of(g * pitch + start, SUB)
        total = acc_a[pl.ds(at, size), :] + acc_b[pl.ds(at, size), :]
        if start == 0:
            wrap = pl.multiple_of(g * pitch + cols, SUB)
            head = total[0:SUB] + (acc_a[pl.ds(wrap, SUB), :] + acc_b[pl.ds(wrap, SUB), :])
            total = jnp.concatenate([head, total[SUB:]], axis=0)
        return total

    chunk = 128
    for start in range(0, cols, chunk):
        edge_ref[0, start:start + chunk, :] = rows_sum(1, start, chunk)
        edge_ref[1, start:start + chunk, :] = rows_sum(groups - 2, start, chunk)
        edge_ref[2, start:start + chunk, :] = rows_sum(0, start, chunk) + rows_sum(groups - 1, start, chunk)
    tab_copy.wait()

    @pl.loop(0, (groups - 4) // 2)
    def _(pair):
        for start in range(0, cols, chunk):
            for side in range(2):
                gbuf[start:start + chunk, side * LANES:(side + 1) * LANES] = rows_sum(2 + 2 * pair + side, start, chunk).astype(BF16)
        column_pass(tab_v, gbuf, h_ref, pair)


def column_pass(tab_v, gbuf, h_ref, pair):
    size = tab_v.shape[1]
    half = size // 2
    lane = lax.broadcasted_iota(jnp.int32, (half, LANES), 1)
    sign = jnp.where(lane < LANES // 2, -1.0, 1.0).astype(F32)
    grid = gbuf[...]
    by_cos = jnp.dot(tab_v[0], grid, preferred_element_type=F32)
    by_sin = jnp.dot(tab_v[1], grid, preferred_element_type=F32)
    for j_half in range(2):
        turned = []
        for side in range(2):
            part = (slice(j_half * half, (j_half + 1) * half), slice(side * LANES, (side + 1) * LANES))
            mixed = by_cos[part] + sign * pltpu.roll(by_sin[part], LANES // 2, 1)
            mixed = jnp.concatenate([mixed, jnp.zeros((LANES - half, LANES), F32)], axis=0)
            turned.append(mixed.T)
        for ch in range(16):
            rows = slice(ch * SUB, (ch + 1) * SUB)
            tile = jnp.concatenate([turned[0][rows], turned[1][rows]], axis=0).astype(BF16)
            if pair is None:
                h_ref[j_half, ch] = tile
            else:
                h_ref[j_half, ch, pl.ds(pl.multiple_of(pair * 16, 16), 16), :] = tile


def image_kernel(h_own, h_oth, e_own, e_oth, tab_hbm, tab2_hbm, maps_hbm, dcol_ref, drow_ref, out_ref,
                 e_v, margins, gbuf, e_turn, tab_v, tab2_v, maps_v, h_all, img, pieces,
                 load_sem, h_load_sem, m_send, m_recv, h_send, h_recv, t_send, t_recv, p_send, p_recv):
    me = lax.axis_index('rows')
    chip = me // 2
    core = me % 2
    peers = [2 * chip + 1 - core, 2 * (1 - chip) + core, 2 * (1 - chip) + 1 - core]
    partner = {'rows': peers[0]}
    block = h_all.shape[2] // 2
    inner = h_own.shape[2]
    half = img.shape[2]

    tab_copy = pltpu.make_async_copy(tab_hbm.at[:, pl.ds(pl.multiple_of(chip * 2 * half, 2 * half), 2 * half), :], tab_v, load_sem.at[0])
    tab2_copy = pltpu.make_async_copy(tab2_hbm, tab2_v, load_sem.at[1])
    maps_copy = pltpu.make_async_copy(maps_hbm, maps_v, load_sem.at[2])
    e_copies = [pltpu.make_async_copy(e.at[0:2], e_v.at[s], load_sem.at[3 + s]) for s, e in enumerate((e_own, e_oth))]
    places = [pl.multiple_of(chip * block, 16), pl.multiple_of((1 - chip) * block, 16)]
    h_copies = [pltpu.make_async_copy(h.at[core], h_all.at[core, :, pl.ds(places[s], inner), :], h_load_sem.at[s]) for s, h in enumerate((h_own, h_oth))]
    for copy in e_copies + [tab_copy] + h_copies + [tab2_copy, maps_copy]:
        copy.start()

    barrier = pltpu.get_barrier_semaphore()
    for peer in peers:
        pl.semaphore_signal(barrier, inc=1, device_id={'rows': peer}, device_id_type=MESH)
    pl.semaphore_wait(barrier, 3)

    m_copies = [pltpu.make_async_remote_copy(src_ref=e.at[2], dst_ref=margins.at[s], send_sem=m_send.at[s], recv_sem=m_recv.at[s], device_id=partner, device_id_type=MESH) for s, e in enumerate((e_own, e_oth))]
    for copy in m_copies:
        copy.start()
    h_sends = [pltpu.make_async_remote_copy(src_ref=h.at[1 - core], dst_ref=h_all.at[core, :, pl.ds(places[s], inner), :], send_sem=h_send.at[s], recv_sem=h_recv.at[s], device_id=partner, device_id_type=MESH) for s, h in enumerate((h_own, h_oth))]
    for copy in h_sends:
        copy.start()

    low = lax.broadcasted_iota(jnp.int32, (128, LANES), 1) % SUB < SUB // 2
    for copy in e_copies + [tab_copy]:
        copy.wait()
    for copy in m_copies:
        copy.wait()
    t_sends = []
    for s in range(2):
        from_low = lax.rem(s + 1 - core, 2)
        from_high = lax.rem(s + core, 2)
        for start in range(0, gbuf.shape[0], 128):
            rows = slice(start, start + 128)
            gbuf[rows, 0:LANES] = (e_v[s, 0, rows, :] + jnp.where(low, margins[from_low, rows, :], 0.0)).astype(BF16)
            gbuf[rows, LANES:2 * LANES] = (e_v[s, 1, rows, :] + jnp.where(low, 0.0, margins[from_high, rows, :])).astype(BF16)
        column_pass(tab_v, gbuf, e_turn.at[s], None)
        edge_place = pl.ds(pl.multiple_of(places[s] + inner, 16), 2 * SUB)
        h_all[core, :, edge_place, :] = e_turn[s, core]
        send = pltpu.make_async_remote_copy(src_ref=e_turn.at[s, 1 - core], dst_ref=h_all.at[core, :, edge_place, :], send_sem=t_send.at[s], recv_sem=t_recv.at[s], device_id=partner, device_id_type=MESH)
        send.start()
        t_sends.append(send)

    rows_half = 2 * half

    def row_pass(parity, i_half, fresh):
        place = pl.ds(pl.multiple_of(i_half * rows_half, rows_half), rows_half)

        @pl.loop(0, 8)
        def _(coil):
            field = jnp.concatenate([h_all[parity, coil], h_all[parity, coil + 8]], axis=1)
            by_cos = jnp.dot(tab2_v[parity, 0, place, :], field, preferred_element_type=F32)
            by_sin = jnp.dot(tab2_v[parity, 1, place, :], field, preferred_element_type=F32)
            img_re = (by_cos[:, :LANES] - by_sin[:, LANES:])[:, :half]
            img_im = (by_sin[:, :LANES] + by_cos[:, LANES:])[:, :half]
            map_re = maps_v[0, coil, place, :]
            map_im = maps_v[1, coil, place, :]
            add_re = map_re * img_re + map_im * img_im
            add_im = map_re * img_im - map_im * img_re
            if fresh:
                first = coil == 0
                img[0, place, :] = jnp.where(first, 0.0, img[0, place, :]) + add_re
                img[1, place, :] = jnp.where(first, 0.0, img[1, place, :]) + add_im
            else:
                img[0, place, :] += add_re
                img[1, place, :] += add_im

    for copy in h_copies + [tab2_copy, maps_copy]:
        copy.wait()
    img[...] = jnp.zeros_like(img)
    row_pass(core, 1 - chip, False)
    row_pass(core, chip, False)
    for copy in h_sends + t_sends:
        copy.wait()
    p_copies = []

    def send_piece(rel):
        target = peers[rel - 1]
        copy = pltpu.make_async_remote_copy(src_ref=img.at[:, pl.ds(pl.multiple_of(target * half, SUB), half), :], dst_ref=pieces.at[rel], send_sem=p_send.at[rel - 1], recv_sem=p_recv.at[rel - 1], device_id={'rows': target}, device_id_type=MESH)
        copy.start()
        p_copies.append(copy)

    row_pass(1 - core, 1 - chip, False)
    send_piece(2)
    send_piece(3)
    row_pass(1 - core, chip, False)
    send_piece(1)
    pieces[0] = img[:, pl.ds(pl.multiple_of(me * half, SUB), half), :]
    for copy in p_copies:
        copy.wait()
    scale = dcol_ref[pl.ds(pl.multiple_of(me * half, SUB), half), :] * drow_ref[...]
    for q in range(2):
        row = []
        for src in range(4):
            rel = lax.rem(src // 2 + chip, 2) * 2 + lax.rem(src % 2 + core, 2)
            row.append(pieces[rel, q])
        out_ref[q] = jnp.concatenate(row, axis=1) * scale


def solution(mesh):
    row_devs = mesh.shape['rows']
    part_axes = ('exam', 'rows')

    def local_step(kspace, weight_row, weight_col, row_idx, col_idx, counts, coil_maps, deapod):
        img_size = deapod.shape[0]
        cols = 2 * img_size
        block_rows = cols // row_devs
        samples = kspace.shape[2]
        pitch = cols + SUB
        half = img_size // row_devs
        groups = block_rows // SUB + 2
        me = lax.axis_index('rows')
        table, table_rows = dft_tables(img_size, row_devs)
        table = jnp.asarray(table)
        table_rows = jnp.asarray(table_rows)

        valid = jnp.arange(samples, dtype=jnp.int32)[None, :] < counts[0]
        place = jnp.clip(row_idx - me * block_rows, 0, block_rows - 1) + (SUB - 3)
        col0 = lax.rem(jnp.clip(col_idx, 0, cols - 1) + (cols - 3), cols)
        addr = (place // SUB) * pitch + col0
        packed = jnp.concatenate([
            kspace.reshape(16, samples),
            jnp.where(valid, weight_row, 0.0),
            (place % SUB).astype(F32)[None, :],
            jnp.zeros((1, samples), F32),
            weight_col,
            addr.astype(F32)[None, :],
            jnp.broadcast_to(counts[0].astype(F32), (1, samples)),
        ], axis=0)
        swap = [(p, (p + row_devs // 2) % row_devs) for p in range(row_devs)]
        packed_other = lax.ppermute(packed, 'rows', swap)

        def grid_block(data):
            return pl.pallas_call(
                functools.partial(grid_kernel, pitch=pitch, cols=cols),
                out_shape=(jax.ShapeDtypeStruct((2, 16, block_rows - 16, LANES), BF16), jax.ShapeDtypeStruct((3, cols, LANES), F32)),
                in_specs=[pl.BlockSpec(memory_space=pltpu.VMEM), pl.BlockSpec(memory_space=pl.ANY)],
                out_specs=(pl.BlockSpec(memory_space=pltpu.VMEM), pl.BlockSpec(memory_space=pltpu.VMEM)),
                scratch_shapes=[
                    pltpu.VMEM((groups * pitch, LANES), F32),
                    pltpu.VMEM((groups * pitch, LANES), F32),
                    pltpu.VMEM((LANES, 2 * LANES), F32),
                    pltpu.VMEM((SUB, samples), jnp.int32),
                    pltpu.VMEM((cols, 2 * LANES), BF16),
                    pltpu.VMEM((2, 2 * half, cols), BF16),
                    pltpu.SMEM((SUB, samples), jnp.int32),
                    pltpu.SemaphoreType.DMA,
                    pltpu.SemaphoreType.DMA,
                ],
                compiler_params=pltpu.CompilerParams(vmem_limit_bytes=40 * 1024 * 1024),
                cost_estimate=pl.CostEstimate(flops=4_000_000_000, bytes_accessed=4_000_000, transcendentals=0),
                name='grid_block',
            )(data, table)

        h_own, e_own = grid_block(packed)
        h_oth, e_oth = grid_block(packed_other)
        any_spec = pl.BlockSpec(memory_space=pl.ANY)
        vmem_spec = pl.BlockSpec(memory_space=pltpu.VMEM)
        return pl.pallas_call(
            image_kernel,
            out_shape=jax.ShapeDtypeStruct((2, half, img_size), F32),
            in_specs=[any_spec] * 7 + [vmem_spec] * 2,
            out_specs=vmem_spec,
            scratch_shapes=[
                pltpu.VMEM((2, 2, cols, LANES), F32),
                pltpu.VMEM((2, cols, LANES), F32),
                pltpu.VMEM((cols, 2 * LANES), BF16),
                pltpu.VMEM((2, 2, 16, 2 * SUB, LANES), BF16),
                pltpu.VMEM((2, 2 * half, cols), BF16),
                pltpu.VMEM((2, 2, img_size, cols // 2), BF16),
                pltpu.VMEM((2, 8, img_size, half), F32),
                pltpu.VMEM((2, 16, 2 * block_rows, LANES), BF16),
                pltpu.VMEM((2, img_size, half), F32),
                pltpu.VMEM((4, 2, half, half), F32),
                pltpu.SemaphoreType.DMA((5,)),
                pltpu.SemaphoreType.DMA((2,)),
                pltpu.SemaphoreType.DMA((2,)),
                pltpu.SemaphoreType.DMA((2,)),
                pltpu.SemaphoreType.DMA((2,)),
                pltpu.SemaphoreType.DMA((2,)),
                pltpu.SemaphoreType.DMA((2,)),
                pltpu.SemaphoreType.DMA((2,)),
                pltpu.SemaphoreType.DMA((3,)),
                pltpu.SemaphoreType.DMA((3,)),
            ],
            compiler_params=pltpu.CompilerParams(collective_id=0, has_side_effects=True, vmem_limit_bytes=40 * 1024 * 1024),
            cost_estimate=pl.CostEstimate(flops=6_000_000_000, bytes_accessed=8_000_000, transcendentals=0),
            name='image_block',
        )(h_own, h_oth, e_own, e_oth, table, table_rows, coil_maps, deapod[:, None], deapod[None, :])

    spec_samples = P(None, part_axes)
    in_specs = (P(None, None, part_axes), spec_samples, spec_samples, P(part_axes), P(part_axes), P(part_axes), P(None, None, None, part_axes), P())
    return jax.shard_map(local_step, mesh=mesh, in_specs=in_specs, out_specs=P(None, part_axes, None), check_vma=False)
```

```python
import functools
import math

import jax
import jax.numpy as jnp
import numpy as np
from jax import lax
from jax.experimental import pallas as pl
from jax.experimental.pallas import tpu as pltpu
from jax.sharding import PartitionSpec as P

MESH = pl.DeviceIdType.MESH
F32 = jnp.float32
BF16 = jnp.bfloat16
LANES = 128
SUB = 8


def dft_tables(img_size, row_devs):
    grid_size = 2 * img_size
    frequency = np.arange(grid_size)[None, :] - img_size
    pixel_pos = np.arange(img_size)[:, None] - img_size // 2
    angle = ((frequency * pixel_pos) % grid_size).astype(np.float64) * (2.0 * math.pi / grid_size)
    table = np.stack([np.cos(angle), np.sin(angle)]).astype(np.float32).astype(jnp.bfloat16)
    block = grid_size // row_devs
    order = np.concatenate([np.arange(SUB, block - SUB), np.arange(SUB), np.arange(block - SUB, block)])
    by_core = []
    for core in range(2):
        rows = np.concatenate([(2 * chip + core) * block + order for chip in range(row_devs // 2)])
        by_core.append(table[:, :, rows])
    by_core = np.stack(by_core)
    by_half = by_core.reshape(2, 2, 2, img_size // 2, grid_size // 2).transpose(0, 2, 1, 3, 4)
    return table, np.ascontiguousarray(by_half.reshape(2, 2, img_size, grid_size // 2))


def pack_kernel(ks_ref, wr_ref, wc_ref, row_ref, col_ref, count_ref, out_ref, *, block_rows, pitch, cols):
    start = lax.axis_index('rows') * block_rows
    count = count_ref[0]
    samples = ks_ref.shape[1]
    valid = lax.broadcasted_iota(jnp.int32, (6, samples), 1) < count
    place = jnp.clip(row_ref[...] - start, 0, block_rows - 1) + (SUB - 3)
    col0 = jnp.clip(col_ref[...], 0, cols - 1) - 3
    col0 = jnp.where(col0 < 0, col0 + cols, col0)
    group = lax.shift_right_logical(place, 3)
    addr = group * pitch + col0
    offset = place - group * SUB
    out_ref[0:16, :] = ks_ref[...]
    out_ref[16:24, :] = jnp.concatenate([jnp.where(valid, wr_ref[...], 0.0), offset.astype(F32), jnp.zeros((1, samples), F32)], axis=0)
    out_ref[24:32, :] = jnp.concatenate([wc_ref[...], addr.astype(F32), jnp.full((1, samples), count, jnp.int32).astype(F32)], axis=0)


def grid_kernel(data_ref, g_ref, edge_ref, acc_a, acc_b, lvec, addr_v, addr_s, addr_sem, *, pitch, cols):
    groups = acc_a.shape[0] // pitch
    addr_v[...] = data_ref[24:32, :].astype(jnp.int32)
    addr_copy = pltpu.make_async_copy(addr_v, addr_s, addr_sem)
    addr_copy.start()

    @pl.loop(0, groups)
    def _(g):
        base = pl.multiple_of(g * pitch, SUB)
        acc_a[pl.ds(base, pitch), :] = jnp.zeros((pitch, LANES), F32)
        acc_b[pl.ds(base, pitch), :] = jnp.zeros((pitch, LANES), F32)

    addr_copy.wait()
    count = addr_s[7, 0]
    slot = lax.broadcasted_iota(jnp.int32, (2 * SUB, LANES), 0).astype(F32)
    tap_row = lax.broadcasted_iota(jnp.int32, (SUB, LANES), 0)

    @pl.loop(0, (count + LANES - 1) // LANES)
    def _(blk):
        first = pl.multiple_of(blk * LANES, LANES)
        wr8 = data_ref[16:24, pl.ds(first, LANES)]
        tap = slot - wr8[6:7, :]
        wrs = jnp.where(tap == 0.0, wr8[0:1, :], 0.0)
        for a in range(1, 6):
            wrs = wrs + jnp.where(tap == float(a), wr8[a:a + 1, :], 0.0)
        y16 = data_ref[0:16, pl.ds(first, LANES)]
        for part in range(2):
            w_part = wrs[part * SUB:(part + 1) * SUB, :]
            full = jnp.concatenate([y16[ch:ch + 1, :] * w_part for ch in range(16)], axis=0)
            lvec[:, part * LANES:(part + 1) * LANES] = full.T
        wc8 = jnp.where(tap_row < 6, data_ref[24:32, pl.ds(first, LANES)], 0.0)

        def contribution(k):
            wide = jnp.broadcast_to(wc8[:, k:k + 1], (SUB, LANES))
            lo = jnp.broadcast_to(lvec[k:k + 1, 0:LANES], (SUB, LANES))
            hi = jnp.broadcast_to(lvec[k:k + 1, LANES:2 * LANES], (SUB, LANES))
            return wide * lo, wide * hi

        for k in range(0, LANES, 2):
            at_a = addr_s[6, first + k]
            at_b = addr_s[6, first + k + 1]
            a_lo, a_hi = contribution(k)
            b_lo, b_hi = contribution(k + 1)
            old_a_lo = acc_a[pl.ds(at_a, SUB), :]
            old_a_hi = acc_a[pl.ds(at_a + pitch, SUB), :]
            old_b_lo = acc_b[pl.ds(at_b, SUB), :]
            old_b_hi = acc_b[pl.ds(at_b + pitch, SUB), :]
            acc_a[pl.ds(at_a, SUB), :] = old_a_lo + a_lo
            acc_a[pl.ds(at_a + pitch, SUB), :] = old_a_hi + a_hi
            acc_b[pl.ds(at_b, SUB), :] = old_b_lo + b_lo
            acc_b[pl.ds(at_b + pitch, SUB), :] = old_b_hi + b_hi

    def rows_sum(g, start, size):
        at = pl.multiple_of(g * pitch + start, SUB)
        total = acc_a[pl.ds(at, size), :] + acc_b[pl.ds(at, size), :]
        if start == 0:
            wrap = pl.multiple_of(g * pitch + cols, SUB)
            head = total[0:SUB] + (acc_a[pl.ds(wrap, SUB), :] + acc_b[pl.ds(wrap, SUB), :])
            total = jnp.concatenate([head, total[SUB:]], axis=0)
        return total

    chunk = 128
    for start in range(0, cols, chunk):
        edge_ref[0, start:start + chunk, :] = rows_sum(1, start, chunk)
        edge_ref[1, start:start + chunk, :] = rows_sum(groups - 2, start, chunk)
        edge_ref[2, start:start + chunk, :] = rows_sum(0, start, chunk) + rows_sum(groups - 1, start, chunk)

    @pl.loop(0, (groups - 4) // 2)
    def _(pair):
        for start in range(0, cols, chunk):
            for side in range(2):
                g_ref[pair, start:start + chunk, side * LANES:(side + 1) * LANES] = rows_sum(2 + 2 * pair + side, start, chunk).astype(BF16)


def image_kernel(g_own, g_oth, e_own, e_oth, tab_ref, tab2_v, maps_r, dcol_ref, drow_ref, out_ref,
                 margins, gbuf_a, gbuf_b, pbuf_a, pbuf_b, tab_v, maps_v, h_all, h_send, img, pieces,
                 m_send, m_recv, s_send, s_recv, p_send, p_recv):
    me = lax.axis_index('rows')
    chip = me // 2
    core = me % 2
    peers = [2 * chip + 1 - core, 2 * (1 - chip) + core, 2 * (1 - chip) + 1 - core]
    partner = {'rows': peers[0]}
    block = h_all.shape[2] // 2
    pairs = g_own.shape[0]
    inner = 2 * SUB * pairs
    half = img.shape[2]
    cols = g_own.shape[1]

    barrier = pltpu.get_barrier_semaphore()
    for peer in peers:
        pl.semaphore_signal(barrier, inc=1, device_id={'rows': peer}, device_id_type=MESH)
    pl.semaphore_wait(barrier, 3)

    m_copies = [pltpu.make_async_remote_copy(src_ref=e.at[2], dst_ref=margins.at[s], send_sem=m_send.at[s], recv_sem=m_recv.at[s], device_id=partner, device_id_type=MESH) for s, e in enumerate((e_own, e_oth))]
    for copy in m_copies:
        copy.start()

    for part in range(2):
        for side, owner in enumerate((me, peers[0])):
            tab_v[(2 * part + side) * half:(2 * part + side + 1) * half, :] = tab_ref[part, pl.ds(pl.multiple_of(owner * half, 2 * SUB), half), :]

    places = [pl.multiple_of(chip * block, 2 * SUB), pl.multiple_of((1 - chip) * block, 2 * SUB)]
    lane = lax.broadcasted_iota(jnp.int32, (half, LANES), 1)
    sign = jnp.where(lane < LANES // 2, -1.0, 1.0).astype(F32)

    def dot_pair(grid, pbuf):
        pbuf[...] = jnp.dot(tab_v[...], grid, preferred_element_type=F32)

    def turn_pair(pbuf, slot, row):
        for j_half in range(2):
            turned = []
            for side in range(2):
                lanes = slice(side * LANES, (side + 1) * LANES)
                by_cos = pbuf[j_half * half:(j_half + 1) * half, lanes]
                by_sin = pbuf[(2 + j_half) * half:(3 + j_half) * half, lanes]
                mixed = by_cos + sign * pltpu.roll(by_sin, LANES // 2, 1)
                mixed = jnp.concatenate([mixed, jnp.zeros((LANES - half, LANES), F32)], axis=0)
                turned.append(mixed.T)
            for ch in range(16):
                rows = slice(ch * SUB, (ch + 1) * SUB)
                tile = jnp.concatenate([turned[0][rows], turned[1][rows]], axis=0).astype(BF16)
                if j_half == 0:
                    h_all[core, ch, pl.ds(pl.multiple_of(places[slot] + row, 2 * SUB), 2 * SUB), :] = tile
                else:
                    h_send[slot, ch, pl.ds(pl.multiple_of(row, 2 * SUB), 2 * SUB), :] = tile

    sends = []

    def send_rows(slot, start, size):
        n = len(sends)
        src = h_send.at[slot, :, start:start + size, :]
        dst = h_all.at[core, :, pl.ds(pl.multiple_of(places[slot] + start, 2 * SUB), size), :]
        copy = pltpu.make_async_remote_copy(src_ref=src, dst_ref=dst, send_sem=s_send.at[n], recv_sem=s_recv.at[n], device_id=partner, device_id_type=MESH)
        copy.start()
        sends.append(copy)

    def close_margins():
        for copy in m_copies:
            copy.wait()
        low = lane[:1] % SUB < SUB // 2
        for s, (e, gbuf) in enumerate(((e_own, gbuf_a), (e_oth, gbuf_b))):
            from_low = lax.rem(s + 1 - core, 2)
            from_high = lax.rem(s + core, 2)
            for start in range(0, cols, 128):
                rows = slice(start, start + 128)
                gbuf[rows, 0:LANES] = (e[0, rows, :] + jnp.where(low, margins[from_low, rows, :], 0.0)).astype(BF16)
                gbuf[rows, LANES:2 * LANES] = (e[1, rows, :] + jnp.where(low, 0.0, margins[from_high, rows, :])).astype(BF16)

    steps = [(g_own, pair, 0, 2 * SUB * pair) for pair in range(pairs)]
    steps += [(gbuf_a, None, 0, inner), (gbuf_b, None, 1, inner)]
    steps += [(g_oth, pair, 1, 2 * SUB * pair) for pair in range(pairs)]
    maps_left = [(q, coil, start) for coil in range(8) for q in range(2) for start in range(0, maps_r.shape[3], LANES)]
    split = 5
    after = {pairs: [(0, 0, inner + 2 * SUB)], pairs + 1 + split: [(1, inner, 2 * SUB), (1, 0, 2 * SUB * split)], 2 * pairs + 1: [(1, 2 * SUB * split, inner - 2 * SUB * split)]}
    bufs = (pbuf_a, pbuf_b)

    def turn_step(n):
        turn_pair(bufs[n % 2], steps[n][2], steps[n][3])
        for where in after.get(n, ()):
            send_rows(*where)

    for n, (grid, pair, slot, row) in enumerate(steps):
        if n == pairs:
            close_margins()
        dot_pair(grid[...] if pair is None else grid[pair], bufs[n % 2])
        for q, coil, start in maps_left[2 * n:2 * n + 2]:
            maps_v[q, coil, start:start + LANES, :] = maps_r[q, coil, :, start:start + LANES].T
        if n:
            turn_step(n - 1)
    turn_step(len(steps) - 1)

    rows_half = 2 * half

    def row_pass(parities, i_half):
        place = pl.ds(pl.multiple_of(i_half * rows_half, rows_half), rows_half)

        def combine(coil):
            pbuf = bufs[coil % 2]
            img_re = (pbuf[:rows_half, :LANES] - pbuf[rows_half:, LANES:])[:, :half]
            img_im = (pbuf[rows_half:, :LANES] + pbuf[:rows_half, LANES:])[:, :half]
            map_re = maps_v[0, coil, place, :]
            map_im = maps_v[1, coil, place, :]
            img[0, place, :] += map_re * img_re + map_im * img_im
            img[1, place, :] += map_re * img_im - map_im * img_re

        for coil in range(8):
            both = 0.0
            for parity in parities:
                field = jnp.concatenate([h_all[parity, coil], h_all[parity, coil + 8]], axis=1)
                both += jnp.dot(tab2_v[parity, i_half], field, preferred_element_type=F32)
            bufs[coil % 2][...] = both
            if coil:
                combine(coil - 1)
        combine(7)

    img[...] = jnp.zeros_like(img)
    row_pass([core], 1 - chip)
    for copy in sends:
        copy.wait()
    p_copies = []

    def send_piece(rel):
        target = peers[rel - 1]
        copy = pltpu.make_async_remote_copy(src_ref=img.at[:, pl.ds(pl.multiple_of(target * half, SUB), half), :], dst_ref=pieces.at[rel], send_sem=p_send.at[rel - 1], recv_sem=p_recv.at[rel - 1], device_id={'rows': target}, device_id_type=MESH)
        copy.start()
        p_copies.append(copy)

    row_pass([1 - core], 1 - chip)
    send_piece(2)
    send_piece(3)
    row_pass([core, 1 - core], chip)
    send_piece(1)
    pieces[0] = img[:, pl.ds(pl.multiple_of(me * half, SUB), half), :]
    for copy in p_copies:
        copy.wait()
    scale = dcol_ref[pl.ds(pl.multiple_of(me * half, SUB), half), :] * drow_ref[...]
    for q in range(2):
        row = []
        for src in range(4):
            rel = lax.rem(src // 2 + chip, 2) * 2 + lax.rem(src % 2 + core, 2)
            row.append(pieces[rel, q])
        out_ref[q] = jnp.concatenate(row, axis=1) * scale


def solution(mesh):
    row_devs = mesh.shape['rows']
    part_axes = ('exam', 'rows')

    def local_step(kspace, weight_row, weight_col, row_idx, col_idx, counts, coil_maps, deapod):
        img_size = deapod.shape[0]
        cols = 2 * img_size
        block_rows = cols // row_devs
        samples = kspace.shape[2]
        pitch = cols + SUB
        half = img_size // row_devs
        groups = block_rows // SUB + 2
        pairs = (groups - 4) // 2
        table, table_rows = dft_tables(img_size, row_devs)
        table = jnp.asarray(table)
        table_rows = jnp.asarray(table_rows)
        vmem_spec = pl.BlockSpec(memory_space=pltpu.VMEM)
        smem_spec = pl.BlockSpec(memory_space=pltpu.SMEM)

        packed = pl.pallas_call(
            functools.partial(pack_kernel, block_rows=block_rows, pitch=pitch, cols=cols),
            out_shape=jax.ShapeDtypeStruct((32, samples), F32),
            in_specs=[vmem_spec] * 5 + [smem_spec],
            out_specs=vmem_spec,
            compiler_params=pltpu.CompilerParams(vmem_limit_bytes=2 * 1024 * 1024),
            name='pack_block',
        )(kspace.reshape(16, samples), weight_row, weight_col, row_idx[None, :], col_idx[None, :], counts)
        swap = [(p, (p + row_devs // 2) % row_devs) for p in range(row_devs)]
        packed_other = lax.ppermute(packed, 'rows', swap)

        def grid_block(data):
            return pl.pallas_call(
                functools.partial(grid_kernel, pitch=pitch, cols=cols),
                out_shape=(jax.ShapeDtypeStruct((pairs, cols, 2 * LANES), BF16), jax.ShapeDtypeStruct((3, cols, LANES), F32)),
                in_specs=[vmem_spec],
                out_specs=(vmem_spec, vmem_spec),
                scratch_shapes=[
                    pltpu.VMEM((groups * pitch, LANES), F32),
                    pltpu.VMEM((groups * pitch, LANES), F32),
                    pltpu.VMEM((LANES, 2 * LANES), F32),
                    pltpu.VMEM((SUB, samples), jnp.int32),
                    pltpu.SMEM((SUB, samples), jnp.int32),
                    pltpu.SemaphoreType.DMA,
                ],
                compiler_params=pltpu.CompilerParams(vmem_limit_bytes=28 * 1024 * 1024),
                cost_estimate=pl.CostEstimate(flops=4_000_000_000, bytes_accessed=4_000_000, transcendentals=0),
                name='grid_block',
            )(data)

        g_own, e_own = grid_block(packed)
        g_oth, e_oth = grid_block(packed_other)
        dma = pltpu.SemaphoreType.DMA
        return pl.pallas_call(
            image_kernel,
            out_shape=jax.ShapeDtypeStruct((2, half, img_size), F32),
            in_specs=[vmem_spec] * 9,
            out_specs=vmem_spec,
            scratch_shapes=[
                pltpu.VMEM((2, cols, LANES), F32),
                pltpu.VMEM((cols, 2 * LANES), BF16),
                pltpu.VMEM((cols, 2 * LANES), BF16),
                pltpu.VMEM((4 * half, 2 * LANES), F32),
                pltpu.VMEM((4 * half, 2 * LANES), F32),
                pltpu.VMEM((4 * half, cols), BF16),
                pltpu.VMEM((2, 8, img_size, half), F32),
                pltpu.VMEM((2, 16, 2 * block_rows, LANES), BF16),
                pltpu.VMEM((2, 16, block_rows, LANES), BF16),
                pltpu.VMEM((2, img_size, half), F32),
                pltpu.VMEM((4, 2, half, half), F32),
                dma((2,)), dma((2,)), dma((4,)), dma((4,)), dma((3,)), dma((3,)),
            ],
            compiler_params=pltpu.CompilerParams(collective_id=0, has_side_effects=True, vmem_limit_bytes=32 * 1024 * 1024),
            cost_estimate=pl.CostEstimate(flops=6_000_000_000, bytes_accessed=8_000_000, transcendentals=0),
            name='image_block',
        )(g_own, g_oth, e_own, e_oth, table, table_rows, jnp.swapaxes(coil_maps, 2, 3), deapod[:, None], deapod[None, :])

    spec_samples = P(None, part_axes)
    in_specs = (P(None, None, part_axes), spec_samples, spec_samples, P(part_axes), P(part_axes), P(part_axes), P(None, None, None, part_axes), P())
    return jax.shard_map(local_step, mesh=mesh, in_specs=in_specs, out_specs=P(None, part_axes, None), check_vma=False)
```
